32 devices in a mesh: member: 4 (over y, x), dom: 8 (over z, core).
Axes of the slice: x: 2, y: 2, z: 4, core: 2. Of those that a mesh axis runs over, the one named last changes fastest.
Arguments:
- acoustic_perturbation: float32 [4, 32, 8192], P('member', None, 'dom'), may hold values from -8 to 8
- prior_acoustic_state: float32 [4, 32, 8192], P('member', None, 'dom'), may hold values from -8 to 8
- thermal_anomaly: float32 [4, 32, 8192], P('member', None, 'dom'), may hold values from -8 to 8
- model_parameters: float32 [4, 4], P('member'), may hold values from 0.5 to 1.5
- crossing_velocity: float32 [32, 24576], P(None, 'dom'), may hold values from -3 to 3
- face_extent: float32 [24576], P('dom'), may hold values from 0.1 to 0.4
- face_metric_factor: float32 [24576], P('dom'), may hold values from 0.01 to 0.06
- reciprocal_polygon_surface: float32 [8192], P('dom'), may hold values from 0.5 to 2
- owned_totals: int32 [8], P('dom'), may hold values from 768 to 1024, as said below
- export_lists: int32 [8, 6, 128], P('dom'), may hold values from 0 to 1024, as said below
- face_neighbour_pair: int32 [2, 24576], P(None, 'dom'), may hold values from 0 to 1792, as said below
- polygon_side_lookup: int32 [6, 8192], P(None, 'dom'), may hold values from 0 to 3072, as said below
Outputs:
- pressure_out: float32 [4, 32, 8192], P('member', None, 'dom')
- temperature_out: float32 [4, 32, 8192], P('member', None, 'dom')
- ensemble_mean: float32 [32, 8192], P(None, 'dom')
The draws below stay inside these ranges and needn't reach their ends.
Inputs may be any that keep to these rules, and one draw needn't show every extreme that they name: The first owned_totals[p] cell slots of partition p are its cells, the rest unused; some partition has 1024. Row export_lists[p, b] lists owned cells of partition p sent to partition (p + offsets[b]) mod 8; filled entries first, then 1024 in the empty slots; at least 64 filled entries a row; in every draw some partition receives 128 filled entries in all 6 of its rows. `face_neighbour_pair`: edge 3 i + j of partition p starts at owned cell i and ends at another owned cell or at halo column 1024 + b * 128 + k whose slot k is filled in the sender's row b; edges of unused cells have both ends at 1792. `polygon_side_lookup`: the local edges with an end at each owned cell, 3072 in empty slots; unused cells have only empty slots.
All inputs are finite; a program needn't handle non-finite values.
Results may differ from the reference program's by a relative error of at most 0.0001.
Values sent between devices are 32-bit elements; how exact they have to be, the bound alone decides.
A program may use at most 64 MiB of HBM per device.

```python
import math
import jax
import jax.numpy as jnp

DOMAIN_CAPACITY = 1024
VERTICAL_LAYERS = 32
HB = 128
NB = 6
MAXE = 6
STEPS = 2
NS = 3
E_DEV = 3072
CELLS = 8192
EDGES = 24576
MEMBERS = 4
N_DOM = 8


def neighbour_offsets_drawn(count):
    return [(block_number // 2 + 1) * (1 - 2 * (block_number % 2)) for block_number in range(count)]


def mesh_tables(key):
    keys = jax.random.split(jax.random.fold_in(key, 7), 9)
    cell_counts = jax.random.randint(keys[0], (N_DOM,), 3 * DOMAIN_CAPACITY // 4, DOMAIN_CAPACITY + 1)
    full_part = jax.random.randint(keys[1], (), 0, N_DOM)
    cell_counts = cell_counts.at[full_part].set(DOMAIN_CAPACITY).astype(jnp.int32)
    offsets = jnp.array(neighbour_offsets_drawn(NB), jnp.int32)
    block_ids = jnp.arange(NB, dtype=jnp.int32)
    filled = jax.random.randint(keys[2], (N_DOM, NB), HB // 2, HB + 1)
    receiver = jax.random.randint(keys[3], (), 0, N_DOM)
    senders = (receiver - offsets) % N_DOM
    filled = filled.at[senders, block_ids].set(HB)
    slot_ids = jnp.arange(HB, dtype=jnp.int32)
    send_raw = jax.random.randint(keys[4], (N_DOM, NB, HB), 0, cell_counts[:, None, None])
    send_table = jnp.where(slot_ids[None, None, :] < filled[:, :, None], send_raw, DOMAIN_CAPACITY).astype(jnp.int32)
    part_ids = jnp.arange(N_DOM, dtype=jnp.int32)
    filled_in = filled[(part_ids[:, None] - offsets[None, :]) % N_DOM, block_ids[None, :]]
    cell_ids = jnp.arange(DOMAIN_CAPACITY, dtype=jnp.int32)
    halo_flag = jax.random.randint(keys[5], (N_DOM, DOMAIN_CAPACITY, 3), 0, 2)
    shifts = jax.random.randint(keys[6], (N_DOM, 3), 1, cell_counts[:, None])
    local_end = (cell_ids[None, :, None] + shifts[:, None, :]) % cell_counts[:, None, None]
    halo_block = jax.random.randint(keys[7], (N_DOM, DOMAIN_CAPACITY, 3), 0, NB)
    block_fill = filled_in[part_ids[:, None, None], halo_block]
    halo_slot = jax.random.randint(keys[8], (N_DOM, DOMAIN_CAPACITY, 3), 0, block_fill)
    halo_end = DOMAIN_CAPACITY + halo_block * HB + halo_slot
    valid = cell_ids[None, :, None] < cell_counts[:, None, None]
    zero_col = DOMAIN_CAPACITY + NB * HB
    start_cell = jnp.where(valid, cell_ids[None, :, None] + 0 * halo_flag, zero_col)
    end_cell = jnp.where(valid, jnp.where(halo_flag == 1, halo_end, local_end), zero_col)
    edge_table = jnp.stack([start_cell.reshape(N_DOM, E_DEV), end_cell.reshape(N_DOM, E_DEV)]).reshape(2, EDGES).astype(jnp.int32)
    side_ids = jnp.arange(3, dtype=jnp.int32)
    outgoing = jnp.where(valid, 3 * cell_ids[None, :, None] + side_ids[None, None, :], E_DEV)
    source = (cell_ids[None, :, None] - shifts[:, None, :]) % cell_counts[:, None, None]
    source_flag = jnp.take_along_axis(halo_flag, source, axis=1)
    incoming = jnp.where(valid & (source_flag == 0), 3 * source + side_ids[None, None, :], E_DEV)
    incidence = jnp.concatenate([outgoing, incoming], axis=2)
    incidence = jnp.transpose(incidence, (2, 0, 1)).reshape(MAXE, CELLS).astype(jnp.int32)
    return (cell_counts, send_table, edge_table, incidence)


def draw_owned_totals(key, part):
    return mesh_tables(key)[0]


def draw_export_lists(key, part):
    return mesh_tables(key)[1]


def draw_face_neighbour_pair(key, part):
    return mesh_tables(key)[2]


def draw_polygon_side_lookup(key, part):
    return mesh_tables(key)[3]


def regional_field(key):
    keys = jax.random.split(key, 2)
    region = 1.5 * jax.random.normal(keys[0], (MEMBERS, 1, N_DOM, 1), jnp.float32)
    noise = jax.random.normal(keys[1], (MEMBERS, VERTICAL_LAYERS, N_DOM, DOMAIN_CAPACITY), jnp.float32)
    return jnp.clip(region + noise, -8.0, 8.0).reshape(MEMBERS, VERTICAL_LAYERS, CELLS)


def draw_acoustic_perturbation(key, part):
    return regional_field(jax.random.fold_in(key, 11))


def draw_prior_acoustic_state(key, part):
    base = regional_field(jax.random.fold_in(key, 11))
    jitter = 0.3 * jax.random.normal(jax.random.fold_in(key, 12), (MEMBERS, VERTICAL_LAYERS, CELLS), jnp.float32)
    return jnp.clip(base + jitter, -8.0, 8.0)


def draw_thermal_anomaly(key, part):
    return regional_field(jax.random.fold_in(key, 13))


def levels(rng, dims, shards, smallest, top_value):
    level, own = 1.0, jax.random.fold_in(rng, 6)
    for dim, parts in shards:
        steps = jnp.exp(jax.random.uniform(jax.random.fold_in(own, dim), (parts,), jnp.float32, smallest / len(shards), top_value / len(shards)))
        level = level * jnp.repeat(steps, dims[dim] // parts).reshape([-1 if axis == dim else 1 for axis in range(len(dims))])
    return level


def centred(stream_key, extent, deviation, most, shards=(), held_as=jnp.bfloat16):
    factor_of = levels(stream_key, extent, shards, -0.22, 0.18) if shards else 1.0
    values = jax.random.normal(stream_key, extent, jnp.float32) * deviation * factor_of
    return jnp.minimum(jnp.maximum(values, -most), most).astype(held_as)


def setup_inputs(seed: int = 0) -> dict:
    key_list = jax.random.split(jax.random.key(seed), 13)
    acoustic_perturbation = draw_acoustic_perturbation(jax.random.fold_in(key_list[12], 71), 0)
    prior_acoustic_state = draw_prior_acoustic_state(jax.random.fold_in(key_list[12], 71), 0)
    thermal_anomaly = draw_thermal_anomaly(jax.random.fold_in(key_list[12], 71), 0)
    model_parameters = jnp.clip(0.5 + 1.0 * jax.random.uniform(key_list[3], (MEMBERS, 4), jnp.float32) ** levels(key_list[3], (MEMBERS, 4), ((0, 4),), -0.2, 0.2), 0.5, 1.5)
    crossing_velocity = centred(key_list[4], (VERTICAL_LAYERS, EDGES), 0.5, 3.0, ((1, 8),), jnp.float32)
    face_extent = jnp.clip(jnp.exp(math.log(0.4) - 1.3862944 * jax.random.uniform(key_list[5], (EDGES,), jnp.float32) ** levels(key_list[5], (EDGES,), ((0, 8),), -0.2, 0.2)), 0.1, 0.4)
    face_metric_factor = jnp.clip(jnp.exp(math.log(0.06) - 1.7917595 * jax.random.uniform(key_list[6], (EDGES,), jnp.float32) ** levels(key_list[6], (EDGES,), ((0, 8),), -0.2, 0.2)), 0.01, 0.06)
    reciprocal_polygon_surface = jnp.clip(jnp.exp(math.log(2.0) - 1.3862944 * jax.random.uniform(key_list[7], (CELLS,), jnp.float32) ** levels(key_list[7], (CELLS,), ((0, 8),), -0.2, 0.2)), 0.5, 2.0)
    owned_totals = draw_owned_totals(jax.random.fold_in(key_list[12], 71), 0)
    export_lists = draw_export_lists(jax.random.fold_in(key_list[12], 71), 0)
    face_neighbour_pair = draw_face_neighbour_pair(jax.random.fold_in(key_list[12], 71), 0)
    polygon_side_lookup = draw_polygon_side_lookup(jax.random.fold_in(key_list[12], 71), 0)
    return dict(acoustic_perturbation=acoustic_perturbation, prior_acoustic_state=prior_acoustic_state, thermal_anomaly=thermal_anomaly, model_parameters=model_parameters, crossing_velocity=crossing_velocity, face_extent=face_extent, face_metric_factor=face_metric_factor, reciprocal_polygon_surface=reciprocal_polygon_surface, owned_totals=owned_totals, export_lists=export_lists, face_neighbour_pair=face_neighbour_pair, polygon_side_lookup=polygon_side_lookup)


time_step = 0.25


def neighbour_offsets(count):
    return [(block_number // 2 + 1) * (1 - 2 * (block_number % 2)) for block_number in range(count)]


def extend_all(fields, export_lists):
    row_count = fields.shape[0]
    zero_column = jnp.zeros((row_count, N_DOM, 1), jnp.float32)
    padded_fields = jnp.concatenate([fields, zero_column], axis=2)
    pieces = [fields]
    for block_number, offset in enumerate(neighbour_offsets(NB)):
        sources = ((jnp.arange(N_DOM, dtype=jnp.int32) - offset) % N_DOM).astype(jnp.int32)
        chosen = export_lists[sources, block_number, :]
        pieces.append(jnp.take_along_axis(padded_fields[:, sources, :], chosen[None], axis=2))
    pieces.append(zero_column)
    return jnp.concatenate(pieces, axis=2)


def at_cells(extended, cell_list):
    return jnp.take_along_axis(extended, cell_list[None], axis=2)


def divergence_all(fluxes, polygon_side_lookup, edge_sign):
    padded_flux = jnp.concatenate([fluxes, jnp.zeros((fluxes.shape[0], N_DOM, 1), jnp.float32)], axis=2)
    summed = jnp.zeros((fluxes.shape[0], N_DOM, DOMAIN_CAPACITY), jnp.float32)
    for corner in range(MAXE):
        summed = summed + edge_sign[corner][None] * at_cells(padded_flux, polygon_side_lookup[corner])
    return summed


def reference(acoustic_perturbation, prior_acoustic_state, thermal_anomaly, model_parameters, crossing_velocity, face_extent, face_metric_factor, reciprocal_polygon_surface, owned_totals, export_lists, face_neighbour_pair, polygon_side_lookup):
    wind = crossing_velocity.reshape(VERTICAL_LAYERS, N_DOM, E_DEV)
    lengths = face_extent.reshape(N_DOM, E_DEV)[None]
    weights = face_metric_factor.reshape(N_DOM, E_DEV)[None]
    inverse = reciprocal_polygon_surface.reshape(N_DOM, DOMAIN_CAPACITY)[None]
    ends = face_neighbour_pair.reshape(2, N_DOM, E_DEV)
    incident = polygon_side_lookup.reshape(MAXE, N_DOM, DOMAIN_CAPACITY)
    cell_ids = jnp.arange(DOMAIN_CAPACITY, dtype=jnp.int32)
    owned = (cell_ids[None, :] < owned_totals[:, None])[None]
    cell_area = jnp.where(owned, 1.0 / inverse, jnp.float32(0.0))
    starts_padded = jnp.concatenate([ends[0], jnp.full((N_DOM, 1), -1, jnp.int32)], axis=1)
    edge_sign = jnp.stack([
        jnp.where(jnp.take_along_axis(starts_padded, incident[corner], axis=1) == cell_ids[None, :], jnp.float32(1.0), jnp.float32(-1.0))
        for corner in range(MAXE)])
    press_list, temp_list = [], []
    for perturbed_run in range(MEMBERS):
        speed = model_parameters[perturbed_run, 0]
        kappa = 0.5 * model_parameters[perturbed_run, 1]
        mixing = 0.6 * model_parameters[perturbed_run, 2]
        couple = model_parameters[perturbed_run, 3]
        current = acoustic_perturbation[perturbed_run].reshape(VERTICAL_LAYERS, N_DOM, DOMAIN_CAPACITY)
        previous = prior_acoustic_state[perturbed_run].reshape(VERTICAL_LAYERS, N_DOM, DOMAIN_CAPACITY)
        scalar_quantity = thermal_anomaly[perturbed_run].reshape(VERTICAL_LAYERS, N_DOM, DOMAIN_CAPACITY)
        for outer_step in range(STEPS):
            theta_ext = extend_all(scalar_quantity, export_lists)
            left = at_cells(theta_ext, ends[0])
            right = at_cells(theta_ext, ends[1])
            fluxes = lengths * (0.5 * wind * (left + right) - (0.5 * jnp.abs(wind) + kappa) * (right - left))
            differences = scalar_quantity[1:] - scalar_quantity[:-1]
            zero_row = jnp.zeros((1, N_DOM, DOMAIN_CAPACITY), jnp.float32)
            vertical = mixing * (jnp.concatenate([differences, zero_row], 0) - jnp.concatenate([zero_row, differences], 0))
            advanced = jnp.where(owned, scalar_quantity + time_step * (-inverse * divergence_all(fluxes, incident, edge_sign) + vertical), scalar_quantity)
            forcing = couple * (advanced - scalar_quantity) / NS
            for substep in range(NS):
                press_ext = extend_all(current, export_lists)
                gradient = weights * (at_cells(press_ext, ends[1]) - at_cells(press_ext, ends[0]))
                stepped = jnp.where(owned, 2.0 * current - previous + speed * inverse * divergence_all(gradient, incident, edge_sign) + forcing, current)
                previous, current = current, stepped
            level_mean = (jnp.sum(current * cell_area, axis=(1, 2)) / jnp.sum(cell_area))[:, None, None]
            current = jnp.where(owned, current - level_mean, current)
            previous = jnp.where(owned, previous - level_mean, previous)
            scalar_quantity = advanced
        press_list.append(current.reshape(VERTICAL_LAYERS, CELLS))
        temp_list.append(scalar_quantity.reshape(VERTICAL_LAYERS, CELLS))
    press_all = jnp.stack(press_list)
    temp_all = jnp.stack(temp_list)
    return press_all, temp_all, jnp.sum(press_all, axis=0) / MEMBERS
```

```python
import functools

import jax
import jax.numpy as jnp
from jax import lax
from jax.experimental import pallas as pl
from jax.experimental.pallas import tpu as pltpu
from jax.sharding import PartitionSpec as P

STEPS = 2
NS = 3
TIME_STEP = 0.25
LANES = 128
MESH = pl.DeviceIdType.MESH
F32 = jnp.float32
BF16 = jnp.bfloat16


def neighbour_offsets(count):
    return [(b // 2 + 1) * (1 - 2 * (b % 2)) for b in range(count)]


def mm(a, b):
    return jnp.dot(a, b, preferred_element_type=F32)


def mm_nt(a, b):
    return lax.dot_general(a, b, (((1,), (1,)), ((), ())), preferred_element_type=F32)


def halves(x):
    high = x.astype(BF16)
    low = (x - high.astype(F32)).astype(BF16)
    return jnp.concatenate([high, low], axis=0)


def fold(x):
    rows = x.shape[0] // 2
    return x[:rows] + x[rows:]


def kernel(
    n,
    members,
    p_ref,
    q_ref,
    t_ref,
    par_ref,
    v_ref,
    ext_ref,
    met_ref,
    inv_ref,
    own_ref,
    exp_ref,
    fin_ref,
    p_out,
    t_out,
    e_out,
    pick,
    g,
    a_hi,
    a_lo,
    b_loc,
    diag,
    xv,
    vj,
    ej,
    send,
    recv,
    mean_send,
    mean_recv,
    mem_send,
    mem_recv,
    mm_send,
    mm_recv,
    send_sem,
    recv_sem,
    mean_ssem,
    mean_rsem,
    mem_ssem,
    mem_rsem,
    mm_ssem,
    mm_rsem,
):
    levels, cells = p_ref.shape[1], p_ref.shape[2]
    slabs = v_ref.shape[1] // cells
    blocks = cells // LANES
    wide = slabs * LANES
    nb = exp_ref.shape[1]
    hb = exp_ref.shape[2]
    halo = nb * hb
    me = lax.axis_index("dom")
    mine = lax.axis_index("member")
    offsets = neighbour_offsets(nb)
    stages = members.bit_length() - 1

    def dom_peer(k):
        return {"dom": lax.rem(me + (k % n), n)}

    def member_peer(stage):
        bit = 1 << stage
        return {"member": mine + bit - 2 * bit * lax.rem(mine // bit, 2)}

    barrier = pltpu.get_barrier_semaphore()
    for k in range(1, n):
        pl.semaphore_signal(barrier, inc=1, device_id=dom_peer(k), device_id_type=MESH)
    for s in range(stages):
        pl.semaphore_signal(barrier, inc=1, device_id=member_peer(s), device_id_type=MESH)

    speed = par_ref[0, 0]
    kappa = 0.5 * par_ref[0, 1]
    mixing = 0.6 * par_ref[0, 2]
    couple = par_ref[0, 3]
    inverse = inv_ref[...]
    owned = lax.broadcasted_iota(jnp.int32, (1, cells), 1) < own_ref[0]
    area = jnp.where(owned, 1.0 / inverse, 0.0)
    started = []

    strip = 16
    sub = lax.broadcasted_iota(jnp.int32, (strip, 1), 0)
    for b in range(nb):
        row = exp_ref[0, b : b + 1, :]

        def build_pick(s, carry, row=row, b=b):
            rows = lax.broadcasted_iota(jnp.int32, (strip, hb), 0) + s * strip
            pick[pl.ds(pl.multiple_of(s * strip, strip), strip), b * hb : (b + 1) * hb] = (
                jnp.where(rows == row, 1.0, 0.0).astype(BF16)
            )
            return carry

        lax.fori_loop(0, cells // strip, build_pick, 0)

    def exchange(slot, chosen):
        copies = []
        for b, offset in enumerate(offsets):
            send[slot, b] = chosen[:, b * hb : (b + 1) * hb]
            copy = pltpu.make_async_remote_copy(
                src_ref=send.at[slot, b],
                dst_ref=recv.at[slot, b],
                send_sem=send_sem.at[slot, b],
                recv_sem=recv_sem.at[slot, b],
                device_id=dom_peer(offset),
                device_id_type=MESH,
            )
            copy.start()
            copies.append(copy)
        started.extend(copies)
        return copies

    def arrived(slot, copies):
        for copy in copies:
            copy.wait_recv()
        return halves(jnp.concatenate([recv[slot, b] for b in range(nb)], axis=1))

    current = p_ref[0]
    previous = q_ref[0]
    theta = t_ref[0]
    xp = halves(current)
    xt = halves(theta)
    both = mm(jnp.concatenate([xt, xp], axis=0), pick[...])
    pl.semaphore_wait(barrier, n - 1 + stages)
    t_copies = exchange(0, fold(both[: 2 * levels]))
    p_copies = exchange(1, fold(both[2 * levels :]))

    base = levels * blocks
    for b in range(blocks):
        cut = slice(b * wide, (b + 1) * wide)
        xv[b * levels : (b + 1) * levels, :] = v_ref[:, cut]
        ends = fin_ref[1:2, cut]
        xv[base + b : base + b + 1, :] = ext_ref[:, cut]
        xv[base + blocks + b : base + blocks + b + 1, :] = met_ref[:, cut]
        xv[base + 2 * blocks + b : base + 2 * blocks + b + 1, :] = (ends // 8).astype(F32)
        xv[base + 3 * blocks + b : base + 3 * blocks + b + 1, :] = (ends % 8).astype(F32)
    ri = lax.broadcasted_iota(jnp.int32, (wide, wide), 0)
    ci = lax.broadcasted_iota(jnp.int32, (wide, wide), 1)
    order = jnp.where(ri == slabs * (ci % LANES) + ci // LANES, 1.0, 0.0).astype(BF16)
    for b in range(blocks):
        y = fold(mm(halves(xv[b * levels : (b + 1) * levels, :]), order))
        for j in range(slabs):
            vj[j, :, b * LANES : (b + 1) * LANES] = y[:, j * LANES : (j + 1) * LANES]
    y = fold(mm(halves(xv[base : base + 4 * blocks, :]), order))
    for kind in range(4):
        for j in range(slabs):
            for b in range(blocks):
                ej[kind * slabs + j : kind * slabs + j + 1, b * LANES : (b + 1) * LANES] = y[
                    kind * blocks + b : kind * blocks + b + 1, j * LANES : (j + 1) * LANES
                ]
    extent = [ej[j : j + 1, :] for j in range(slabs)]
    metric = [ej[slabs + j : slabs + j + 1, :] for j in range(slabs)]
    ends = [
        8.0 * ej[2 * slabs + j : 2 * slabs + j + 1, :] + ej[3 * slabs + j : 3 * slabs + j + 1, :]
        for j in range(slabs)
    ]

    def strip_of(s):
        at = pl.ds(pl.multiple_of(s * strip, strip), strip)
        rows = (lax.broadcasted_iota(jnp.int32, (strip, cells), 0) + s * strip).astype(F32)
        total = jnp.zeros((strip, cells), F32)
        for j in range(slabs):
            hit = rows == ends[j]
            g[at, j * cells : (j + 1) * cells] = jnp.where(hit, 1.0, 0.0).astype(BF16)
            total = total + jnp.where(hit, metric[j], 0.0)
        return at, total

    def put(at, value, columns):
        high = value.astype(BF16)
        a_hi[at, columns] = high
        a_lo[at, columns] = (value - high.astype(F32)).astype(BF16)

    def build_local(s, carry):
        at, total = strip_of(s)
        b_loc[at, :] = total
        return carry

    def build_halo(s, carry):
        at, total = strip_of(s)
        put(at, total, slice(None))
        diag[...] += total
        return carry

    diag[...] = jnp.zeros_like(diag)
    lax.fori_loop(0, cells // strip, build_local, 0)
    lax.fori_loop(cells // strip, (cells + halo) // strip, build_halo, 0)

    def symmetric(i, carry):
        at = pl.ds(pl.multiple_of(i * LANES, LANES), LANES)
        for j in range(blocks):
            cut = slice(j * LANES, (j + 1) * LANES)
            value = b_loc[at, cut] + b_loc[cut, at].T
            put(at, value, cut)
            total = value[:strip]
            for r in range(1, LANES // strip):
                total = total + value[r * strip : (r + 1) * strip]
            diag[:, cut] += total
        return carry

    lax.fori_loop(0, blocks, symmetric, 0)
    degree = jnp.sum(diag[...], axis=0, keepdims=True)
    scale = speed * inverse

    def far_local(x, j):
        return fold(mm(x, g[:cells, j * cells : (j + 1) * cells]))

    def far_halo(x, j):
        return fold(mm(x, g[cells:, j * cells : (j + 1) * cells]))

    def slab_flux(theta, far, j):
        wind = vj[j]
        flux = extent[j] * (
            0.5 * wind * (theta + far) - (0.5 * jnp.abs(wind) + kappa) * (far - theta)
        )
        incoming = mm_nt(halves(flux), g[:cells, j * cells : (j + 1) * cells])
        return flux - fold(incoming)

    def theta_end(theta, div):
        step = theta[1:] - theta[:-1]
        zero = jnp.zeros((1, cells), F32)
        vertical = mixing * (
            jnp.concatenate([step, zero], 0) - jnp.concatenate([zero, step], 0)
        )
        advanced = jnp.where(owned, theta + TIME_STEP * (vertical - inverse * div), theta)
        return advanced, couple * (advanced - theta) / NS

    def local_part(x):
        return fold(mm(x, a_hi[:cells, :])) + mm(x[:levels], a_lo[:cells, :])

    def halo_part(x):
        return fold(mm(x, a_hi[cells:, :])) + mm(x[:levels], a_lo[cells:, :])

    def partial_mean(slot, field):
        weighted = jnp.sum(field * area, axis=1, keepdims=True)
        whole = jnp.sum(area, axis=1, keepdims=True)
        row_at = lax.broadcasted_iota(jnp.int32, (levels, LANES), 0)
        lane_at = lax.broadcasted_iota(jnp.int32, (levels, LANES), 1)
        row = jnp.sum(jnp.where(row_at == lane_at, weighted, 0.0), axis=0, keepdims=True)
        lane = lax.broadcasted_iota(jnp.int32, (1, LANES), 1)
        row = jnp.where(lane < levels, row, whole)
        mean_send[slot] = jnp.broadcast_to(row, (8, LANES))
        copies = []
        for k in range(1, n):
            copy = pltpu.make_async_remote_copy(
                src_ref=mean_send.at[slot],
                dst_ref=mean_recv.at[slot, k - 1],
                send_sem=mean_ssem.at[slot, k - 1],
                recv_sem=mean_rsem.at[slot, k - 1],
                device_id=dom_peer(k),
                device_id_type=MESH,
            )
            copy.start()
            copies.append(copy)
        started.extend(copies)
        return copies

    def mean_row(slot, copies):
        total = mean_send[slot]
        for k, copy in enumerate(copies):
            copy.wait_recv()
            total = total + mean_recv[slot, k]
        return total / total[:, levels : levels + 1]

    def as_column(row):
        row_at = lax.broadcasted_iota(jnp.int32, (levels, LANES), 0)
        lane_at = lax.broadcasted_iota(jnp.int32, (levels, LANES), 1)
        return jnp.sum(jnp.where(row_at == lane_at, row[0:1], 0.0), axis=1, keepdims=True)

    ht = arrived(0, t_copies)
    div = jnp.zeros((levels, cells), F32)
    for j in range(slabs):
        div = div + slab_flux(theta, far_local(xt, j) + far_halo(ht, j), j)
    theta1, forcing = theta_end(theta, div)
    xt1 = halves(theta1)

    mean_copies = None
    slot = 1
    total_substeps = STEPS * NS
    div = jnp.zeros((levels, cells), F32)
    ht1 = None
    for k in range(total_substeps):
        accel = local_part(xp) - degree * current
        if k == NS - 1:
            ht1 = arrived(0 + STEPS * NS + 1, t_copies)
            for j in range(slabs - 1):
                div = div + slab_flux(theta1, far_local(xt1, j) + far_halo(ht1, j), j)
        if k == NS:
            mean_copies = partial_mean(0, current)
            j = slabs - 1
            div = div + slab_flux(theta1, far_local(xt1, j) + far_halo(ht1, j), j)
            theta2, forcing = theta_end(theta1, div)
            t_out[0] = theta2
        accel = accel + halo_part(arrived(slot, p_copies))
        stepped = jnp.where(
            owned, 2.0 * current - previous + scale * accel + forcing, current
        )
        previous, current = current, stepped
        if k < total_substeps - 1:
            slot += 1
            xp = halves(current)
            p_copies = exchange(slot, fold(mm(xp, pick[...])))
            if k == 0:
                t_copies = exchange(STEPS * NS + 1, fold(mm(xt1, pick[...])))

    first = as_column(mean_row(0, mean_copies))
    current = jnp.where(owned, current - first, current)

    width = cells // max(stages, 1)
    last_copies = partial_mean(1, current)
    e_out[...] = current

    def member_stage(stage):
        copies = []
        for c in range(stages):
            cut = slice(c * width, (c + 1) * width)
            mem_send[stage, c] = e_out[:, cut]
            copy = pltpu.make_async_remote_copy(
                src_ref=mem_send.at[stage, c],
                dst_ref=mem_recv.at[stage, c],
                send_sem=mem_ssem.at[stage, c],
                recv_sem=mem_rsem.at[stage, c],
                device_id=member_peer((stage + c) % stages),
                device_id_type=MESH,
            )
            copy.start()
            copies.append(copy)
        started.extend(copies)
        return copies

    def member_add(stage, copies):
        for c, copy in enumerate(copies):
            cut = slice(c * width, (c + 1) * width)
            copy.wait_recv()
            e_out[:, cut] = mem_send[stage, c] + mem_recv[stage, c]

    bulk = member_stage(0) if stages else []
    last = mean_row(1, last_copies)
    summed = last
    p_out[0] = jnp.where(owned, current - as_column(last), current)
    for s in range(stages):
        mm_send[s] = summed
        copy = pltpu.make_async_remote_copy(
            src_ref=mm_send.at[s],
            dst_ref=mm_recv.at[s],
            send_sem=mm_ssem.at[s],
            recv_sem=mm_rsem.at[s],
            device_id=member_peer(s),
            device_id_type=MESH,
        )
        copy.start()
        started.append(copy)
        member_add(s, bulk)
        if s + 1 < stages:
            bulk = member_stage(s + 1)
        copy.wait_recv()
        summed = mm_send[s] + mm_recv[s]
    e_out[...] = (e_out[...] - jnp.where(owned, as_column(summed), 0.0)) / members
    for copy in started:
        copy.wait_send()


def solution(mesh):
    n = mesh.shape["dom"]
    members = mesh.shape["member"]

    def per_device(
        acoustic_perturbation,
        prior_acoustic_state,
        thermal_anomaly,
        model_parameters,
        crossing_velocity,
        face_extent,
        face_metric_factor,
        reciprocal_polygon_surface,
        owned_totals,
        export_lists,
        face_neighbour_pair,
        polygon_side_lookup,
    ):
        _, levels, cells = acoustic_perturbation.shape
        edges = face_extent.shape[0]
        slabs = edges // cells
        blocks = cells // LANES
        nb, hb = export_lists.shape[1:]
        halo = nb * hb
        stages = members.bit_length() - 1
        some = max(stages, 1)
        slots = STEPS * NS + 2
        vmem = pl.BlockSpec(memory_space=pltpu.VMEM)
        smem = pl.BlockSpec(memory_space=pltpu.SMEM)
        dma = pltpu.SemaphoreType.DMA
        return pl.pallas_call(
            functools.partial(kernel, n, members),
            out_shape=(
                jax.ShapeDtypeStruct((1, levels, cells), F32),
                jax.ShapeDtypeStruct((1, levels, cells), F32),
                jax.ShapeDtypeStruct((levels, cells), F32),
            ),
            in_specs=[vmem, vmem, vmem, smem, vmem, vmem, vmem, vmem, smem, vmem, vmem],
            out_specs=(vmem, vmem, vmem),
            scratch_shapes=[
                pltpu.VMEM((cells, halo), BF16),
                pltpu.VMEM((cells + halo, edges), BF16),
                pltpu.VMEM((cells + halo, cells), BF16),
                pltpu.VMEM((cells + halo, cells), BF16),
                pltpu.VMEM((cells, cells), F32),
                pltpu.VMEM((16, cells), F32),
                pltpu.VMEM((levels * blocks + 4 * blocks, slabs * LANES), F32),
                pltpu.VMEM((slabs, levels, cells), F32),
                pltpu.VMEM((16, cells), F32),
                pltpu.VMEM((slots, nb, levels, hb), F32),
                pltpu.VMEM((slots, nb, levels, hb), F32),
                pltpu.VMEM((STEPS, 8, LANES), F32),
                pltpu.VMEM((STEPS, n - 1, 8, LANES), F32),
                pltpu.VMEM((some, some, levels, cells // some), F32),
                pltpu.VMEM((some, some, levels, cells // some), F32),
                pltpu.VMEM((some, 8, LANES), F32),
                pltpu.VMEM((some, 8, LANES), F32),
                dma((slots, nb)),
                dma((slots, nb)),
                dma((STEPS, n - 1)),
                dma((STEPS, n - 1)),
                dma((some, some)),
                dma((some, some)),
                dma((some,)),
                dma((some,)),
            ],
            compiler_params=pltpu.CompilerParams(
                collective_id=0, has_side_effects=True, vmem_limit_bytes=60 * 1024 * 1024
            ),
        )(
            acoustic_perturbation,
            prior_acoustic_state,
            thermal_anomaly,
            model_parameters,
            crossing_velocity,
            face_extent[None],
            face_metric_factor[None],
            reciprocal_polygon_surface[None],
            owned_totals,
            export_lists,
            face_neighbour_pair,
        )

    in_specs = (
        P("member", None, "dom"),
        P("member", None, "dom"),
        P("member", None, "dom"),
        P("member", None),
        P(None, "dom"),
        P("dom"),
        P("dom"),
        P("dom"),
        P("dom"),
        P("dom", None, None),
        P(None, "dom"),
        P(None, "dom"),
    )
    out_specs = (P("member", None, "dom"), P("member", None, "dom"), P(None, "dom"))
    return jax.shard_map(
        per_device, mesh=mesh, in_specs=in_specs, out_specs=out_specs, check_vma=False
    )
```
